32 devices in a mesh: vocab: 8 (over y, x, core), hid: 4 (over z).
Axes of the slice: x: 2, y: 2, z: 4, core: 2. Of those that a mesh axis runs over, the one named last changes fastest.
Arguments:
- hidden: bfloat16 [2, 256, 7168], P(None, 'vocab', 'hid'), may hold values from -100 to 100
- head_weight: bfloat16 [7168, 65536], P('hid', 'vocab'), may hold values from -2 to 2
- targets: int32 [2, 256], P(None, 'hid'), may hold values from 0 to 65535
Outputs:
- entropy: float32 [2, 256], P(None, 'hid')
- squared: float32 [2, 256], P(None, 'hid')
The draws below stay inside these ranges and needn't reach their ends.
All inputs are finite; a program needn't handle non-finite values.
Results may differ from the reference program's by a relative error of at most 0.0003.
Values may be sent and summed in bfloat16 or wider, within the bound.
A program may use at most 192 MiB of HBM per device.

```python
import math
import jax
import jax.numpy as jnp

D = 7168
DEPTH = 2
VOCAB = 65536
TOKENS = 256


def column_block(key, index):
    block_key = jax.random.fold_in(jax.random.fold_in(key, 7001), index)
    column_ids = index * 128 + jnp.arange(128)
    column_ramp = 1.0 + 0.25 * column_ids.astype(jnp.float32) / VOCAB
    raw_values = jnp.clip(jax.random.normal(block_key, (D, 128), jnp.float32), -6.0, 6.0)
    return raw_values * column_ramp[None, :] / math.sqrt(D)


def draw_head_weight(key, part):
    blocks = jax.vmap(lambda index: column_block(key, index))(jnp.arange(VOCAB // 128))
    return jnp.transpose(blocks, (1, 0, 2)).reshape(D, VOCAB).astype(jnp.bfloat16)


def draw_hidden(key, part):
    hidden_key = jax.random.fold_in(key, 7002)
    base_values = 3.0 * jnp.clip(jax.random.normal(hidden_key, (DEPTH, TOKENS, D), jnp.float32), -6.0, 6.0)
    return jnp.clip(base_values, -100.0, 100.0).astype(jnp.bfloat16)


def touch_ends(result, rng, smallest, high):
    longest = result.shape.index(max(result.shape))
    spots = []
    for shift in (0, 1):
        where = [jax.random.randint(jax.random.fold_in(rng, axis), (), 0, length) for axis, length in enumerate(result.shape)]
        where[longest] = (where[longest] + shift) % result.shape[longest]
        spots.append(tuple(where))
    return result.at[spots[0]].set(smallest).at[spots[1]].set(high)


def setup_inputs(seed: int = 0) -> dict:
    key_of = jax.random.split(jax.random.key(seed), 4)
    hidden = draw_hidden(jax.random.fold_in(key_of[3], 71), 0)
    head_weight = draw_head_weight(jax.random.fold_in(key_of[3], 71), 0)
    targets = touch_ends(jax.random.randint(key_of[2], (DEPTH, TOKENS), 0, VOCAB), jax.random.fold_in(key_of[2], 1), 0, VOCAB - 1).astype(jnp.int32)
    return dict(hidden=hidden, head_weight=head_weight, targets=targets)


def reference(hidden, head_weight, targets):
    entropy_rows = []
    square_rows = []
    for depth_index in range(DEPTH):
        logits = jnp.dot(hidden[depth_index], head_weight, preferred_element_type=jnp.float32)
        row_peak = jnp.max(logits, axis=1)
        row_total = jnp.sum(jnp.exp(logits - row_peak[:, None]), axis=1)
        log_norm = row_peak + jnp.log(row_total)
        picked = jnp.take_along_axis(logits, targets[depth_index][:, None], axis=1)[:, 0]
        entropy_rows.append(log_norm - picked)
        square_rows.append(log_norm * log_norm)
    return jnp.stack(entropy_rows), jnp.stack(square_rows)
```

```python
import functools

import jax
import jax.numpy as jnp
from jax import lax
from jax.experimental import pallas as pl
from jax.experimental.pallas import tpu as pltpu
from jax.sharding import PartitionSpec as P

MESH = pl.DeviceIdType.MESH
LANES = 128
SKEW = 3
AHEAD = 3
LOWEST = -3.0e38
TOP = 32767.0


def kernel(
    n, nv, nj, cw, ring,
    hidden, weight, targets,
    out,
    rows, wbuf, came, gone, came_scale, gone_scale, part,
    labels, label_tile, peak, mass, pick, ends, mine, shared,
    w_sem, own_sem, h_send, h_recv, l_send, l_recv,
    q_send, q_recv, s_send, s_recv, e_send, e_recv, c_send, c_recv,
):
    v, me = lax.axis_index("vocab"), lax.axis_index("hid")
    groups = nv // 2
    chip, parity = v // 2, v % 2
    depths, share, width = hidden.shape
    block = depths * share
    half = nj * cw
    span = 2 * nj
    units = nv * nj
    columns = [slice(c * LANES, (c + 1) * LANES) for c in range(cw // LANES)]
    low = me < n // 2
    ways = (jnp.where(low, 0, 1), jnp.where(low, 1, 0))
    near = jnp.where(low, me, n - 1 - me)
    places = (near, n - 1 - near)
    nexts = (jnp.where(low, me + 1, me - 1), jnp.where(low, me - 1, me + 1))

    def w_copy(t, j):
        return pltpu.make_async_copy(
            weight.at[:, pl.ds(pl.multiple_of(ways[t] * half + j * cw, cw), cw)],
            wbuf.at[ways[t] * nj + j],
            w_sem.at[t * nj + j],
        )

    own = pltpu.make_async_copy(hidden, rows.at[chip, parity], own_sem)
    own.start()
    w_copy(0, 0).start()

    barrier = pltpu.get_barrier_semaphore()
    for k in range(1, nv):
        pl.semaphore_signal(barrier, inc=1, device_id=((v + k) % nv, me), device_id_type=MESH)
    for k in range(1, n):
        pl.semaphore_signal(barrier, inc=1, device_id=(v, (me + k) % n), device_id_type=MESH)

    for j in range(1, AHEAD):
        w_copy(0, j).start()
    for j in range(AHEAD - 1):
        w_copy(1, j).start()

    def h_copy(target):
        return pltpu.make_async_remote_copy(
            src_ref=hidden, dst_ref=rows.at[chip, parity], send_sem=h_send, recv_sem=h_recv.at[v],
            device_id=(target, me), device_id_type=MESH,
        )

    def h_arrival(g, side):
        return pltpu.make_async_remote_copy(
            src_ref=hidden, dst_ref=rows.at[g, side], send_sem=h_send, recv_sem=h_recv.at[2 * g + side],
            device_id=(v, me), device_id_type=MESH,
        )

    def small_dot(t, u):
        j = u % nj
        a = rows[chip, (v + u // nj) % 2].reshape(block, width)
        part[t, u % 2] = jnp.dot(a, wbuf[ways[t] * nj + j], preferred_element_type=jnp.float32)

    def group_of(u):
        return (chip + u // span) % groups

    def dot(t, u):
        @pl.when(u < span)
        def _():
            @pl.when(u < nj)
            def _():
                @pl.when(u + AHEAD - 1 < nj)
                def _():
                    w_copy(t, u + AHEAD - 1).start()

                w_copy(t, u).wait()

            if t == 0:
                @pl.when(u == nj)
                def _():
                    h_arrival(chip, 1 - parity).wait_recv()

            small_dot(t, u)

        @pl.when(jnp.logical_and(jnp.logical_and(u >= span, u < units), u % 2 == 0))
        def _():
            g = group_of(u)
            if t == 0:
                @pl.when(u % span == 0)
                def _():
                    for side in range(2):
                        h_arrival(g, side).wait_recv()

            a = rows[g].reshape(2 * block, width)
            y = jnp.dot(a, wbuf[ways[t] * nj + (u % span) // 2], preferred_element_type=jnp.float32)
            part[t] = y.reshape(2, block, cw)

    own.wait()
    w_copy(0, 0).wait()
    small_dot(0, 0)
    pl.semaphore_wait(barrier, nv - 1 + n - 1)

    peers = [2 * chip + 1 - parity]
    for back in range(1, groups):
        other = (chip - back + groups) % groups
        peers += [2 * other + parity, 2 * other + 1 - parity]
    for target in peers:
        h_copy(target).start()

    finals = (n - 1, 0)

    def l_copy(e):
        return pltpu.make_async_remote_copy(
            src_ref=targets, dst_ref=labels.at[me], send_sem=l_send.at[e], recv_sem=l_recv.at[me],
            device_id=(v, finals[e]), device_id_type=MESH,
        )

    for e in range(2):
        @pl.when(me != finals[e])
        def _():
            l_copy(e).start()

        @pl.when(me == finals[e])
        def _():
            labels[me] = targets[...]

    def message(t, u, target):
        way = ways[t]
        data = pltpu.make_async_remote_copy(
            src_ref=gone.at[way, u], dst_ref=came.at[way, u],
            send_sem=q_send.at[way], recv_sem=q_recv.at[way, u % ring],
            device_id=(v, target), device_id_type=MESH,
        )
        scale = pltpu.make_async_remote_copy(
            src_ref=gone_scale.at[way, u], dst_ref=came_scale.at[way, u],
            send_sem=s_send.at[way], recv_sem=s_recv.at[way, u % ring],
            device_id=(v, target), device_id_type=MESH,
        )
        return scale, data

    def send_end(e, g):
        return pltpu.make_async_remote_copy(
            src_ref=ends.at[g], dst_ref=mine.at[e], send_sem=e_send.at[g], recv_sem=e_recv.at[e],
            device_id=(v, g), device_id_type=MESH,
        )

    def held(t, u):
        return [part[t, u % 2, :, c] for c in columns]

    def received(t, u):
        for copy in message(t, u, me):
            copy.wait_recv()
        scale = came_scale[ways[t], u]
        return [
            part[t, u % 2, :, c] + came[ways[t], u, :, c].astype(jnp.int32).astype(jnp.float32) * scale
            for c in columns
        ]

    def ship(t, u, pieces):
        largest = functools.reduce(jnp.maximum, [jnp.abs(piece) for piece in pieces])
        largest = jnp.maximum(jnp.max(largest, axis=0, keepdims=True), 1e-30)
        gone_scale[ways[t], u] = largest * (1.0 / TOP)
        up = TOP / largest
        for c, piece in zip(columns, pieces):
            gone[ways[t], u, :, c] = jnp.round(piece * up).astype(jnp.int32).astype(jnp.int16)
        for copy in message(t, u, nexts[t]):
            copy.start()

    def order(line):
        return jnp.concatenate(
            [line[a : a + 1, s * share : (s + 1) * share] for s in range(2) for a in range(depths)], axis=1
        )

    def statistics(u, pieces):
        g, r = group_of(u), u % span

        @pl.when(u == 0)
        def _():
            for z in range(n):
                @pl.when(me != z)
                def _():
                    pltpu.make_async_remote_copy(
                        src_ref=targets, dst_ref=labels.at[z], send_sem=l_send.at[0], recv_sem=l_recv.at[z],
                        device_id=(v, me), device_id_type=MESH,
                    ).wait_recv()

        @pl.when(r == 0)
        def _():
            label_tile[...] = jnp.transpose(jnp.broadcast_to(order(labels[g]), (LANES, 2 * block)))
            peak[...] = jnp.full_like(peak, LOWEST)
            mass[...] = jnp.zeros_like(mass)
            pick[...] = jnp.zeros_like(pick)

        first_group = u < span
        side = jnp.where(first_group, (v + u // nj) % 2, r % 2)
        j = jnp.where(first_group, u % nj, r // 2)
        here = pl.ds(pl.multiple_of(side * block, block), block)
        old = peak[here, :]
        new = functools.reduce(jnp.maximum, pieces, old)
        peak[here, :] = new
        mass[here, :] = mass[here, :] * jnp.exp(old - new) + sum(jnp.exp(piece - new) for piece in pieces)
        offset = label_tile[here, :] - (v * (2 * half) + ways[1] * half + j * cw)
        lane = lax.broadcasted_iota(jnp.int32, (block, LANES), 1)
        found = pick[here, :]
        for c, piece in enumerate(pieces):
            found = found + jnp.where(offset == lane + c * LANES, piece, 0.0)
        pick[here, :] = found

        @pl.when(r == span - 1)
        def _():
            tall = jnp.transpose(peak[...])
            top = jnp.max(tall, axis=0, keepdims=True)
            weight_sum = jnp.sum(jnp.transpose(mass[...]) * jnp.exp(tall - top), axis=0, keepdims=True)
            chosen = jnp.sum(jnp.transpose(pick[...]), axis=0, keepdims=True)
            ends[g] = jnp.concatenate(
                [top, weight_sum, chosen, jnp.zeros((5, 2 * block), jnp.float32)], axis=0
            )

            @pl.when(g != me)
            def _():
                send_end(ways[1], g).start()

            @pl.when(g == me)
            def _():
                mine[ways[1]] = ends[g]

    def step(i, carry):
        u = i - places[0] * SKEW

        @pl.when(jnp.logical_and(u >= 0, u < units))
        def _():
            @pl.when(places[0] == 0)
            def _():
                ship(0, u, held(0, u))

            @pl.when(places[0] > 0)
            def _():
                ship(0, u, received(0, u))

            dot(0, u + 1)

        w = i - places[1] * SKEW

        @pl.when(jnp.logical_and(w >= 0, w < units))
        def _():
            @pl.when(places[1] < n - 1)
            def _():
                ship(1, w, received(1, w))

            @pl.when(places[1] == n - 1)
            def _():
                statistics(w, received(1, w))

        @pl.when(jnp.logical_and(w >= -1, w < units))
        def _():
            dot(1, w + 1)

        return carry

    lax.fori_loop(0, units + (n - 1) * SKEW, step, 0)

    for e in range(2):
        @pl.when(me != finals[e])
        def _():
            send_end(e, me).wait_recv()

    def merge(tiles):
        top = functools.reduce(jnp.maximum, [t[0:1] for t in tiles])
        weight_sum = sum(t[1:2] * jnp.exp(t[0:1] - top) for t in tiles)
        chosen = sum(t[2:3] for t in tiles)
        return top, weight_sum, chosen

    top, weight_sum, chosen = merge([mine[0], mine[1]])
    shared[v] = jnp.concatenate([top, weight_sum, chosen, jnp.zeros((5, 2 * block), jnp.float32)], axis=0)

    def c_copy(slot, source, target):
        return pltpu.make_async_remote_copy(
            src_ref=shared.at[source], dst_ref=shared.at[source], send_sem=c_send.at[slot], recv_sem=c_recv.at[source],
            device_id=(target, me), device_id_type=MESH,
        )

    for k in range(1, nv):
        c_copy(k - 1, v, (v + k) % nv).start()

    for _ in range(nv - 1):
        h_copy(v).wait_send()
    for e in range(2):
        @pl.when(me != finals[e])
        def _():
            l_copy(e).wait_send()
    for t in range(2):
        @pl.when(places[t] < n - 1)
        def _():
            pltpu.make_async_copy(gone.at[ways[t]], came.at[ways[t]], q_send.at[ways[t]]).wait()
            pltpu.make_async_copy(gone_scale.at[ways[t]], came_scale.at[ways[t]], s_send.at[ways[t]]).wait()

    @pl.when(places[1] == n - 1)
    def _():
        for g in range(groups):
            @pl.when(me != g)
            def _():
                send_end(ways[1], g).wait_send()

    for k in range(1, nv):
        c_copy(0, (v + k) % nv, v).wait_recv()
    top, weight_sum, chosen = merge([shared[k] for k in range(nv)])
    norm = top + jnp.log(weight_sum)
    for b, line in enumerate((norm, chosen)):
        for a in range(depths):
            out[depths * b + a : depths * b + a + 1, :] = jnp.concatenate(
                [line[:, (s * depths + a) * share : (s * depths + a + 1) * share] for s in range(2)], axis=1
            )

    for k in range(1, nv):
        c_copy(k - 1, v, (v + k) % nv).wait_send()


def body(n, nv, hidden, head_weight, targets):
    depths, share, width = hidden.shape
    columns = head_weight.shape[1]
    groups = nv // 2
    assert groups == n and n >= 2 and depths * 2 * share == LANES
    cw = min(512, columns // 2)
    nj = columns // 2 // cw
    units = nv * nj
    block = depths * share
    ring = 16
    while ring < (n - 1) * SKEW + 4:
        ring *= 2
    vmem, anywhere = pl.BlockSpec(memory_space=pltpu.VMEM), pl.BlockSpec(memory_space=pl.ANY)
    dma = pltpu.SemaphoreType.DMA
    result = pl.pallas_call(
        functools.partial(kernel, n, nv, nj, cw, ring),
        out_shape=jax.ShapeDtypeStruct((2 * depths, targets.shape[1]), jnp.float32),
        in_specs=[anywhere, anywhere, vmem],
        out_specs=vmem,
        scratch_shapes=[
            pltpu.VMEM((groups, 2, depths, share, width), hidden.dtype),
            pltpu.VMEM((2 * nj, width, cw), head_weight.dtype),
            pltpu.VMEM((2, units, block, cw), jnp.int16),
            pltpu.VMEM((2, units, block, cw), jnp.int16),
            pltpu.VMEM((2, units, 1, LANES), jnp.float32),
            pltpu.VMEM((2, units, 1, LANES), jnp.float32),
            pltpu.VMEM((2, 2, block, cw), jnp.float32),
            pltpu.VMEM((n,) + targets.shape, jnp.int32),
            pltpu.VMEM((2 * block, LANES), jnp.int32),
            pltpu.VMEM((2 * block, LANES), jnp.float32),
            pltpu.VMEM((2 * block, LANES), jnp.float32),
            pltpu.VMEM((2 * block, LANES), jnp.float32),
            pltpu.VMEM((groups, 8, 2 * block), jnp.float32),
            pltpu.VMEM((2, 8, 2 * block), jnp.float32),
            pltpu.VMEM((nv, 8, 2 * block), jnp.float32),
            dma((2 * nj,)), dma, dma, dma((nv,)), dma((2,)), dma((n,)),
            dma((2,)), dma((2, ring)), dma((2,)), dma((2, ring)),
            dma((groups,)), dma((2,)), dma((nv - 1,)), dma((nv,)),
        ],
        compiler_params=pltpu.CompilerParams(
            collective_id=0, has_side_effects=True, vmem_limit_bytes=60 * 1024 * 1024
        ),
    )(hidden, head_weight, targets)
    norm, chosen = result[:depths], result[depths:]
    return norm - chosen, norm * norm


def solution(mesh):
    return jax.shard_map(
        functools.partial(body, mesh.shape["hid"], mesh.shape["vocab"]),
        mesh=mesh,
        in_specs=(P(None, "vocab", "hid"), P("hid", "vocab"), P(None, "hid")),
        out_specs=(P(None, "hid"), P(None, "hid")),
        check_vma=False,
    )
```

```python
import functools

import jax
import jax.numpy as jnp
from jax import lax
from jax.experimental import pallas as pl
from jax.experimental.pallas import tpu as pltpu
from jax.sharding import PartitionSpec as P

MESH = pl.DeviceIdType.MESH
LANES = 128
SKEW = 3
AHEAD = 3
BACK = 2
LOWEST = -3.0e38
TOP = 32767.0


def kernel(
    n, nv, nj, cw, ring,
    hidden, weight, targets,
    out,
    rows, wbuf, came, gone, came_scale, gone_scale, part,
    labels, label_tile, peak, mass, pick, ends, mine, shared, late,
    w_sem, own_sem, h_send, h_recv, l_send, l_recv,
    q_send, q_recv, s_send, s_recv, e_send, e_recv, c_send, c_recv, t_send, t_recv,
):
    v, me = lax.axis_index("vocab"), lax.axis_index("hid")
    groups = nv // 2
    chip, parity = v // 2, v % 2
    depths, share, width = hidden.shape
    block = depths * share
    half = nj * cw
    span = 2 * nj
    units = nv * nj
    columns = [slice(c * LANES, (c + 1) * LANES) for c in range(cw // LANES)]
    low = me < n // 2
    ways = (jnp.where(low, 0, 1), jnp.where(low, 1, 0))
    near = jnp.where(low, me, n - 1 - me)
    places = (near, n - 1 - near)
    nexts = (jnp.where(low, me + 1, me - 1), jnp.where(low, me - 1, me + 1))

    kept = units - BACK
    ending = (0, 1, n - 2, n - 1)

    def last_group(c):
        return n // 2 - 1 + c % 2

    def w_copy(t, j):
        return pltpu.make_async_copy(
            weight.at[:, pl.ds(pl.multiple_of(ways[t] * half + j * cw, cw), cw)],
            wbuf.at[ways[t] * nj + j],
            w_sem.at[t * nj + j],
        )

    own = pltpu.make_async_copy(hidden, rows.at[chip, parity], own_sem)
    own.start()
    w_copy(0, 0).start()
    row = lax.broadcasted_iota(jnp.int32, (8, 2 * block), 0)
    neutral = jnp.where(row == 0, LOWEST, 0.0)
    for k in range(nv):
        shared[k] = neutral
        for e in range(len(ending)):
            late[k, e] = neutral

    barrier = pltpu.get_barrier_semaphore()
    for k in range(1, nv):
        pl.semaphore_signal(barrier, inc=1, device_id=((v + k) % nv, me), device_id_type=MESH)
    for k in range(1, n):
        pl.semaphore_signal(barrier, inc=1, device_id=(v, (me + k) % n), device_id_type=MESH)

    for j in range(1, AHEAD):
        w_copy(0, j).start()
    for j in range(AHEAD - 1):
        w_copy(1, j).start()

    def h_copy(target):
        return pltpu.make_async_remote_copy(
            src_ref=hidden, dst_ref=rows.at[chip, parity], send_sem=h_send, recv_sem=h_recv.at[v],
            device_id=(target, me), device_id_type=MESH,
        )

    def h_arrival(g, side):
        return pltpu.make_async_remote_copy(
            src_ref=hidden, dst_ref=rows.at[g, side], send_sem=h_send, recv_sem=h_recv.at[2 * g + side],
            device_id=(v, me), device_id_type=MESH,
        )

    def small_dot(t, u):
        j = u % nj
        a = rows[chip, (v + u // nj) % 2].reshape(block, width)
        part[t, u % 2] = jnp.dot(a, wbuf[ways[t] * nj + j], preferred_element_type=jnp.float32)

    def group_of(u):
        turn = u // span
        natural, final = (chip + turn) % groups, last_group(chip)
        other = jnp.where(natural == final, (chip + groups - 1) % groups, natural)
        return jnp.where(turn == groups - 1, final, other)

    def big_dot(t, g, chunk):
        a = rows[g].reshape(2 * block, width)
        y = jnp.dot(a, wbuf[chunk], preferred_element_type=jnp.float32)
        part[t] = y.reshape(2, block, cw)

    def dot(t, u):
        @pl.when(u < span)
        def _():
            @pl.when(u < nj)
            def _():
                @pl.when(u + AHEAD - 1 < nj)
                def _():
                    w_copy(t, u + AHEAD - 1).start()

                w_copy(t, u).wait()

            if t == 0:
                @pl.when(u == nj)
                def _():
                    h_arrival(chip, 1 - parity).wait_recv()

            small_dot(t, u)

        @pl.when(jnp.logical_and(jnp.logical_and(u >= span, u < units), u % 2 == 0))
        def _():
            g = group_of(u)
            if t == 0:
                @pl.when(u % span == 0)
                def _():
                    for side in range(2):
                        h_arrival(g, side).wait_recv()

            big_dot(t, g, ways[t] * nj + (u % span) // 2)

        if t == 0:
            @pl.when(jnp.logical_and(u == units, places[0] == 0))
            def _():
                big_dot(0, last_group(chip), ways[1] * nj + nj - 1)

    own.wait()
    w_copy(0, 0).wait()
    small_dot(0, 0)
    pl.semaphore_wait(barrier, nv - 1 + n - 1)

    peers = [2 * chip + 1 - parity]
    for back in range(1, groups):
        other = (chip - back + groups) % groups
        peers += [2 * other + parity, 2 * other + 1 - parity]
    for target in peers:
        h_copy(target).start()

    finals = (n - 1, 0)

    def l_copy(e):
        return pltpu.make_async_remote_copy(
            src_ref=targets, dst_ref=labels.at[me], send_sem=l_send.at[e], recv_sem=l_recv.at[me],
            device_id=(v, ending[e]), device_id_type=MESH,
        )

    for e in range(len(ending)):
        @pl.when(me != ending[e])
        def _():
            l_copy(e).start()

        @pl.when(me == ending[e])
        def _():
            labels[me] = targets[...]

    def message(t, u, target):
        way = ways[t]
        data = pltpu.make_async_remote_copy(
            src_ref=gone.at[way, u], dst_ref=came.at[way, u],
            send_sem=q_send.at[way], recv_sem=q_recv.at[way, u % ring],
            device_id=(v, target), device_id_type=MESH,
        )
        scale = pltpu.make_async_remote_copy(
            src_ref=gone_scale.at[way, u], dst_ref=came_scale.at[way, u],
            send_sem=s_send.at[way], recv_sem=s_recv.at[way, u % ring],
            device_id=(v, target), device_id_type=MESH,
        )
        return scale, data

    def send_end(e, g):
        return pltpu.make_async_remote_copy(
            src_ref=ends.at[g], dst_ref=mine.at[e], send_sem=e_send.at[g], recv_sem=e_recv.at[e],
            device_id=(v, g), device_id_type=MESH,
        )

    def held(t, u):
        return [part[t, u % 2, :, c] for c in columns]

    def received(t, u):
        for copy in message(t, u, me):
            copy.wait_recv()
        scale = came_scale[ways[t], u]
        return [
            part[t, u % 2, :, c] + came[ways[t], u, :, c].astype(jnp.int32).astype(jnp.float32) * scale
            for c in columns
        ]

    def returned(u):
        for copy in message(0, u, me):
            copy.wait_recv()
        scale = came_scale[ways[0], u]
        return [came[ways[0], u, :, c].astype(jnp.int32).astype(jnp.float32) * scale for c in columns]

    def late_copy(e, target):
        return pltpu.make_async_remote_copy(
            src_ref=ends.at[last_group(chip)], dst_ref=late.at[v, e], send_sem=t_send, recv_sem=t_recv.at[v, e],
            device_id=(target, last_group(chip)), device_id_type=MESH,
        )

    def late_arrival(k, e):
        return pltpu.make_async_remote_copy(
            src_ref=ends.at[0], dst_ref=late.at[k, e], send_sem=t_send, recv_sem=t_recv.at[k, e],
            device_id=(v, me), device_id_type=MESH,
        )

    def ship(t, u, pieces):
        largest = functools.reduce(jnp.maximum, [jnp.abs(piece) for piece in pieces])
        largest = jnp.maximum(jnp.max(largest, axis=0, keepdims=True), 1e-30)
        gone_scale[ways[t], u] = largest * (1.0 / TOP)
        up = TOP / largest
        for c, piece in zip(columns, pieces):
            gone[ways[t], u, :, c] = jnp.round(piece * up).astype(jnp.int32).astype(jnp.int16)
        for copy in message(t, u, nexts[t]):
            copy.start()

    def order(line):
        return jnp.concatenate(
            [line[a : a + 1, s * share : (s + 1) * share] for s in range(2) for a in range(depths)], axis=1
        )

    def statistics(u, pieces, start, stop):
        g, r = group_of(u), u % span

        @pl.when(u == start)
        def _():
            for z in range(n):
                @pl.when(me != z)
                def _():
                    pltpu.make_async_remote_copy(
                        src_ref=targets, dst_ref=labels.at[z], send_sem=l_send.at[0], recv_sem=l_recv.at[z],
                        device_id=(v, me), device_id_type=MESH,
                    ).wait_recv()

        @pl.when(jnp.logical_or(r == 0, u == start))
        def _():
            label_tile[...] = jnp.transpose(jnp.broadcast_to(order(labels[g]), (LANES, 2 * block)))
            peak[...] = jnp.full_like(peak, LOWEST)
            mass[...] = jnp.zeros_like(mass)
            pick[...] = jnp.zeros_like(pick)

        first_group = u < span
        side = jnp.where(first_group, (v + u // nj) % 2, r % 2)
        j = jnp.where(first_group, u % nj, r // 2)
        here = pl.ds(pl.multiple_of(side * block, block), block)
        old = peak[here, :]
        new = functools.reduce(jnp.maximum, pieces, old)
        peak[here, :] = new
        mass[here, :] = mass[here, :] * jnp.exp(old - new) + sum(jnp.exp(piece - new) for piece in pieces)
        offset = label_tile[here, :] - (v * (2 * half) + ways[1] * half + j * cw)
        lane = lax.broadcasted_iota(jnp.int32, (block, LANES), 1)
        found = pick[here, :]
        for c, piece in enumerate(pieces):
            found = found + jnp.where(offset == lane + c * LANES, piece, 0.0)
        pick[here, :] = found

        @pl.when(jnp.logical_or(r == span - 1, u == stop - 1))
        def _():
            tall = jnp.transpose(peak[...])
            top = jnp.max(tall, axis=0, keepdims=True)
            weight_sum = jnp.sum(jnp.transpose(mass[...]) * jnp.exp(tall - top), axis=0, keepdims=True)
            chosen = jnp.sum(jnp.transpose(pick[...]), axis=0, keepdims=True)
            ends[g] = jnp.concatenate(
                [top, weight_sum, chosen, jnp.zeros((5, 2 * block), jnp.float32)], axis=0
            )

            @pl.when(u == stop - 1)
            def _():
                for e in range(len(ending)):
                    @pl.when(me == ending[e])
                    def _():
                        @pl.when(me == last_group(chip))
                        def _():
                            late[v, e] = ends[last_group(chip)]

                        for k in range(nv):
                            @pl.when(jnp.logical_or(me != last_group(chip), v != k))
                            def _():
                                late_copy(e, k).start()

            @pl.when(jnp.logical_and(u != stop - 1, g != me))
            def _():
                send_end(ways[1], g).start()

            @pl.when(jnp.logical_and(u != stop - 1, g == me))
            def _():
                mine[ways[1]] = ends[g]

    def step(i, carry):
        u = i - places[0] * SKEW
        extra = jnp.where(places[0] == 0, BACK, 0)

        @pl.when(jnp.logical_and(u >= 0, u < units + extra))
        def _():
            @pl.when(places[0] == 0)
            def _():
                ship(0, u, held(0, u))

            @pl.when(places[0] > 0)
            def _():
                ship(0, u, received(0, u))

        w = i - places[1] * SKEW

        @pl.when(jnp.logical_and(w >= 0, w < units))
        def _():
            @pl.when(jnp.logical_and(places[1] < n - 1, jnp.logical_or(w < kept, places[1] < n - 2)))
            def _():
                ship(1, w, received(1, w))

            @pl.when(jnp.logical_and(places[1] == n - 1, w < kept))
            def _():
                statistics(w, received(1, w), 0, kept)

            @pl.when(jnp.logical_and(places[1] == n - 2, w >= kept))
            def _():
                total = [a + b for a, b in zip(received(1, w), returned(w + BACK))]
                statistics(w, total, kept, units)

        @pl.when(jnp.logical_and(u >= 0, u < units))
        def _():
            dot(0, u + 1)

        @pl.when(jnp.logical_and(w >= -1, w < jnp.where(places[1] == n - 1, kept, units) - 1))
        def _():
            dot(1, w + 1)

        return carry

    lax.fori_loop(0, units + (n - 1) * SKEW, step, 0)

    def merge(tiles):
        top = functools.reduce(jnp.maximum, [t[0:1] for t in tiles])
        weight_sum = sum(t[1:2] * jnp.exp(t[0:1] - top) for t in tiles)
        chosen = sum(t[2:3] for t in tiles)
        return top, weight_sum, chosen

    def c_copy(slot, source, target):
        return pltpu.make_async_remote_copy(
            src_ref=shared.at[source], dst_ref=shared.at[source], send_sem=c_send.at[slot], recv_sem=c_recv.at[source],
            device_id=(target, me), device_id_type=MESH,
        )

    early = last_group(chip) != me

    @pl.when(early)
    def _():
        for e in range(2):
            @pl.when(me != finals[e])
            def _():
                send_end(e, me).wait_recv()

        top, weight_sum, chosen = merge([mine[0], mine[1]])
        shared[v] = jnp.concatenate([top, weight_sum, chosen, jnp.zeros((5, 2 * block), jnp.float32)], axis=0)
        for k in range(1, nv):
            c_copy(k - 1, v, (v + k) % nv).start()

    for _ in range(nv - 1):
        h_copy(v).wait_send()
    for e in range(len(ending)):
        @pl.when(me != ending[e])
        def _():
            l_copy(e).wait_send()

    def sent(t, count):
        way = ways[t]
        pltpu.make_async_copy(gone.at[way, 0:count], came.at[way, 0:count], q_send.at[way]).wait()
        pltpu.make_async_copy(gone_scale.at[way, 0:count], came_scale.at[way, 0:count], s_send.at[way]).wait()

    for t, role, count in (
        (0, places[0] == 0, units + BACK), (0, places[0] > 0, units),
        (1, places[1] < n - 2, units), (1, places[1] == n - 2, kept),
    ):
        @pl.when(role)
        def _():
            sent(t, count)

    @pl.when(places[1] == n - 1)
    def _():
        for g in range(groups):
            @pl.when(jnp.logical_and(me != g, g != last_group(chip)))
            def _():
                send_end(ways[1], g).wait_send()

    @pl.when(places[1] >= n - 2)
    def _():
        for k in range(nv):
            @pl.when(jnp.logical_or(me != last_group(chip), v != k))
            def _():
                late_copy(0, k).wait_send()

    for k in range(nv):
        @pl.when(jnp.logical_and(last_group(k // 2) != me, v != k))
        def _():
            c_copy(0, k, v).wait_recv()

        for e in range(len(ending)):
            @pl.when(jnp.logical_and(last_group(k // 2) == me, jnp.logical_or(v != k, me != ending[e])))
            def _():
                late_arrival(k, e).wait_recv()

    top, weight_sum, chosen = merge(
        [shared[k] for k in range(nv)] + [late[k, e] for k in range(nv) for e in range(len(ending))]
    )
    norm = top + jnp.log(weight_sum)
    for b, line in enumerate((norm, chosen)):
        for a in range(depths):
            out[depths * b + a : depths * b + a + 1, :] = jnp.concatenate(
                [line[:, (s * depths + a) * share : (s * depths + a + 1) * share] for s in range(2)], axis=1
            )

    @pl.when(early)
    def _():
        for k in range(1, nv):
            c_copy(k - 1, v, (v + k) % nv).wait_send()


def body(n, nv, hidden, head_weight, targets):
    depths, share, width = hidden.shape
    columns = head_weight.shape[1]
    groups = nv // 2
    assert groups == n and n >= 4 and depths * 2 * share == LANES
    cw = min(512, columns // 2)
    nj = columns // 2 // cw
    units = nv * nj
    block = depths * share
    ring = 16
    while ring < (n - 1) * SKEW + 4:
        ring *= 2
    vmem, anywhere = pl.BlockSpec(memory_space=pltpu.VMEM), pl.BlockSpec(memory_space=pl.ANY)
    dma = pltpu.SemaphoreType.DMA
    result = pl.pallas_call(
        functools.partial(kernel, n, nv, nj, cw, ring),
        out_shape=jax.ShapeDtypeStruct((2 * depths, targets.shape[1]), jnp.float32),
        in_specs=[anywhere, anywhere, vmem],
        out_specs=vmem,
        scratch_shapes=[
            pltpu.VMEM((groups, 2, depths, share, width), hidden.dtype),
            pltpu.VMEM((2 * nj, width, cw), head_weight.dtype),
            pltpu.VMEM((2, units + BACK, block, cw), jnp.int16),
            pltpu.VMEM((2, units + BACK, block, cw), jnp.int16),
            pltpu.VMEM((2, units + BACK, 1, LANES), jnp.float32),
            pltpu.VMEM((2, units + BACK, 1, LANES), jnp.float32),
            pltpu.VMEM((2, 2, block, cw), jnp.float32),
            pltpu.VMEM((n,) + targets.shape, jnp.int32),
            pltpu.VMEM((2 * block, LANES), jnp.int32),
            pltpu.VMEM((2 * block, LANES), jnp.float32),
            pltpu.VMEM((2 * block, LANES), jnp.float32),
            pltpu.VMEM((2 * block, LANES), jnp.float32),
            pltpu.VMEM((groups, 8, 2 * block), jnp.float32),
            pltpu.VMEM((2, 8, 2 * block), jnp.float32),
            pltpu.VMEM((nv, 8, 2 * block), jnp.float32),
            pltpu.VMEM((nv, 4, 8, 2 * block), jnp.float32),
            dma((2 * nj,)), dma, dma, dma((nv,)), dma((4,)), dma((n,)),
            dma((2,)), dma((2, ring)), dma((2,)), dma((2, ring)),
            dma((groups,)), dma((2,)), dma((nv - 1,)), dma((nv,)), dma, dma((nv, 4)),
        ],
        compiler_params=pltpu.CompilerParams(
            collective_id=0, has_side_effects=True, vmem_limit_bytes=60 * 1024 * 1024
        ),
    )(hidden, head_weight, targets)
    norm, chosen = result[:depths], result[depths:]
    return norm - chosen, norm * norm


def solution(mesh):
    return jax.shard_map(
        functools.partial(body, mesh.shape["hid"], mesh.shape["vocab"]),
        mesh=mesh,
        in_specs=(P(None, "vocab", "hid"), P("hid", "vocab"), P(None, "hid")),
        out_specs=(P(None, "hid"), P(None, "hid")),
        check_vma=False,
    )
```

```python
import functools

import jax
import jax.numpy as jnp
from jax import lax
from jax.experimental import pallas as pl
from jax.experimental.pallas import tpu as pltpu
from jax.sharding import PartitionSpec as P

MESH = pl.DeviceIdType.MESH
LANES = 128
SKEW = 3
AHEAD = 3
BACK = 2
LOWEST = -3.0e38
TOP = 32767.0


def kernel(
    n, nv, nj, cw, ring,
    hidden, weight, targets,
    out,
    rows, wbuf, came, gone, came_scale, gone_scale, part,
    labels, label_tile, peak, mass, pick, ends, mine, shared, late,
    w_sem, own_sem, label_sem, h_send, h_recv, l_send, l_recv,
    q_send, q_recv, s_send, s_recv, e_send, e_recv, c_send, c_recv, t_send, t_recv,
):
    v, me = lax.axis_index("vocab"), lax.axis_index("hid")
    groups = nv // 2
    chip, parity = v // 2, v % 2
    depths, share, width = hidden.shape
    block = depths * share
    half = nj * cw
    span = 2 * nj
    units = nv * nj
    columns = [slice(c * LANES, (c + 1) * LANES) for c in range(cw // LANES)]
    low = me < n // 2
    ways = (jnp.where(low, 0, 1), jnp.where(low, 1, 0))
    near = jnp.where(low, me, n - 1 - me)
    places = (near, n - 1 - near)
    nexts = (jnp.where(low, me + 1, me - 1), jnp.where(low, me - 1, me + 1))

    kept = units - BACK
    ending = (0, 1, n - 2, n - 1)

    def last_group(c):
        return n // 2 - 1 + c % 2

    def w_copy(t, j):
        return pltpu.make_async_copy(
            weight.at[:, pl.ds(pl.multiple_of(ways[t] * half + j * cw, cw), cw)],
            wbuf.at[ways[t] * nj + j],
            w_sem.at[t, j % (AHEAD + 1)],
        )

    own = pltpu.make_async_copy(hidden, rows.at[chip, parity], own_sem)
    own.start()
    w_copy(0, 0).start()
    row = lax.broadcasted_iota(jnp.int32, (8, 2 * block), 0)
    neutral = jnp.where(row == 0, LOWEST, 0.0)
    for k in range(nv):
        shared[k] = neutral
    for k in range(late.shape[0]):
        late[k] = neutral

    barrier = pltpu.get_barrier_semaphore()
    for k in range(1, nv):
        pl.semaphore_signal(barrier, inc=1, device_id=((v + k) % nv, me), device_id_type=MESH)
    for k in range(1, n):
        pl.semaphore_signal(barrier, inc=1, device_id=(v, (me + k) % n), device_id_type=MESH)

    for j in range(1, AHEAD):
        w_copy(0, j).start()
    for j in range(AHEAD - 1):
        w_copy(1, j).start()

    def h_copy(target):
        return pltpu.make_async_remote_copy(
            src_ref=hidden, dst_ref=rows.at[chip, parity], send_sem=h_send, recv_sem=h_recv.at[v],
            device_id=(target, me), device_id_type=MESH,
        )

    def h_arrival(g, side):
        return pltpu.make_async_remote_copy(
            src_ref=hidden, dst_ref=rows.at[g, side], send_sem=h_send, recv_sem=h_recv.at[2 * g + side],
            device_id=(v, me), device_id_type=MESH,
        )

    def small_dot(t, u):
        j = u % nj
        a = rows[chip, (v + u // nj) % 2].reshape(block, width)
        part[t, u % 2] = jnp.dot(a, wbuf[ways[t] * nj + j], preferred_element_type=jnp.float32)

    def group_of(u):
        turn = u // span
        natural, final = (chip + turn) % groups, last_group(chip)
        other = jnp.where(natural == final, (chip + groups - 1) % groups, natural)
        return jnp.where(turn == groups - 1, final, other)

    def big_dot(t, g, chunk):
        a = rows[g].reshape(2 * block, width)
        y = jnp.dot(a, wbuf[chunk], preferred_element_type=jnp.float32)
        part[t] = y.reshape(2, block, cw)

    def dot(t, u):
        @pl.when(u < span)
        def _():
            @pl.when(u < nj)
            def _():
                @pl.when(u + AHEAD - 1 < nj)
                def _():
                    w_copy(t, u + AHEAD - 1).start()

                w_copy(t, u).wait()

            if t == 0:
                @pl.when(u == nj)
                def _():
                    h_arrival(chip, 1 - parity).wait_recv()

            small_dot(t, u)

        @pl.when(jnp.logical_and(jnp.logical_and(u >= span, u < units), u % 2 == 0))
        def _():
            g = group_of(u)
            if t == 0:
                @pl.when(u % span == 0)
                def _():
                    for side in range(2):
                        h_arrival(g, side).wait_recv()

            big_dot(t, g, ways[t] * nj + (u % span) // 2)

        if t == 0:
            @pl.when(jnp.logical_and(u == units, places[0] == 0))
            def _():
                big_dot(0, last_group(chip), ways[1] * nj + nj - 1)

    finals = (n - 1, 0)

    def l_copy(e):
        return pltpu.make_async_remote_copy(
            src_ref=targets, dst_ref=labels.at[me], send_sem=l_send, recv_sem=l_recv,
            device_id=(v, ending[e]), device_id_type=MESH,
        )

    def message(t, u, target):
        way = ways[t]
        data = pltpu.make_async_remote_copy(
            src_ref=gone.at[way, u], dst_ref=came.at[way, u],
            send_sem=q_send.at[way], recv_sem=q_recv.at[way, u % ring],
            device_id=(v, target), device_id_type=MESH,
        )
        scale = pltpu.make_async_remote_copy(
            src_ref=gone_scale.at[way, u], dst_ref=came_scale.at[way, u],
            send_sem=s_send.at[way], recv_sem=s_recv.at[way, u % ring],
            device_id=(v, target), device_id_type=MESH,
        )
        return scale, data

    def send_end(e, g):
        return pltpu.make_async_remote_copy(
            src_ref=ends.at[g], dst_ref=mine.at[e], send_sem=e_send, recv_sem=e_recv.at[e],
            device_id=(v, g), device_id_type=MESH,
        )

    def held(t, u):
        return [part[t, u % 2, :, c] for c in columns]

    def received(t, u):
        for copy in message(t, u, me):
            copy.wait_recv()
        scale = came_scale[ways[t], u]
        return [
            part[t, u % 2, :, c] + came[ways[t], u, :, c].astype(jnp.int32).astype(jnp.float32) * scale
            for c in columns
        ]

    def returned(u):
        for copy in message(0, u, me):
            copy.wait_recv()
        scale = came_scale[ways[0], u]
        return [came[ways[0], u, :, c].astype(jnp.int32).astype(jnp.float32) * scale for c in columns]

    def late_place(e):
        return (chip // 2 * 2 + parity) * len(ending) + e

    def late_copy(e, target):
        return pltpu.make_async_remote_copy(
            src_ref=ends.at[last_group(chip)], dst_ref=late.at[late_place(e)], send_sem=t_send, recv_sem=t_recv,
            device_id=(target, last_group(chip)), device_id_type=MESH,
        )

    def prepare(t, u, pieces):
        largest = functools.reduce(jnp.maximum, [jnp.abs(piece) for piece in pieces])
        largest = jnp.maximum(jnp.max(largest, axis=0, keepdims=True), 1e-30)
        gone_scale[ways[t], u] = largest * (1.0 / TOP)
        up = TOP / largest
        for c, piece in zip(columns, pieces):
            gone[ways[t], u, :, c] = jnp.round(piece * up).astype(jnp.int32).astype(jnp.int16)

    def launch(t, u):
        for copy in message(t, u, nexts[t]):
            copy.start()

    def ship(t, u, pieces):
        prepare(t, u, pieces)
        launch(t, u)

    own.wait()
    w_copy(0, 0).wait()
    small_dot(0, 0)

    @pl.when(places[0] == 0)
    def _():
        prepare(0, 0, held(0, 0))

    pl.semaphore_wait(barrier, nv - 1 + n - 1)

    @pl.when(places[0] == 0)
    def _():
        launch(0, 0)

    peers = [2 * chip + 1 - parity]
    for back in range(1, groups):
        other = (chip - back + groups) % groups
        peers += [2 * other + parity, 2 * other + 1 - parity]
    for target in peers:
        h_copy(target).start()

    for e in range(len(ending)):
        @pl.when(me != ending[e])
        def _():
            l_copy(e).start()

    own_labels = pltpu.make_async_copy(targets, labels.at[me], label_sem)
    own_labels.start()

    def order(line):
        return jnp.concatenate(
            [line[a : a + 1, s * share : (s + 1) * share] for s in range(2) for a in range(depths)], axis=1
        )

    def statistics(u, pieces, start, stop):
        g, r = group_of(u), u % span

        @pl.when(u == start)
        def _():
            pltpu.make_async_copy(labels.at[0 : n - 1], labels.at[1:n], l_recv).wait()
            pltpu.make_async_copy(targets, labels.at[me], label_sem).wait()

        @pl.when(jnp.logical_or(r == 0, u == start))
        def _():
            label_tile[...] = jnp.transpose(jnp.broadcast_to(order(labels[g]), (LANES, 2 * block)))
            peak[...] = jnp.full_like(peak, LOWEST)
            mass[...] = jnp.zeros_like(mass)
            pick[...] = jnp.zeros_like(pick)

        first_group = u < span
        side = jnp.where(first_group, (v + u // nj) % 2, r % 2)
        j = jnp.where(first_group, u % nj, r // 2)
        here = pl.ds(pl.multiple_of(side * block, block), block)
        old = peak[here, :]
        new = functools.reduce(jnp.maximum, pieces, old)
        peak[here, :] = new
        mass[here, :] = mass[here, :] * jnp.exp(old - new) + sum(jnp.exp(piece - new) for piece in pieces)
        offset = label_tile[here, :] - (v * (2 * half) + ways[1] * half + j * cw)
        lane = lax.broadcasted_iota(jnp.int32, (block, LANES), 1)
        found = pick[here, :]
        for c, piece in enumerate(pieces):
            found = found + jnp.where(offset == lane + c * LANES, piece, 0.0)
        pick[here, :] = found

        @pl.when(jnp.logical_or(r == span - 1, u == stop - 1))
        def _():
            tall = jnp.transpose(peak[...])
            top = jnp.max(tall, axis=0, keepdims=True)
            weight_sum = jnp.sum(jnp.transpose(mass[...]) * jnp.exp(tall - top), axis=0, keepdims=True)
            chosen = jnp.sum(jnp.transpose(pick[...]), axis=0, keepdims=True)
            ends[g] = jnp.concatenate(
                [top, weight_sum, chosen, jnp.zeros((5, 2 * block), jnp.float32)], axis=0
            )

            @pl.when(u == stop - 1)
            def _():
                for e in range(len(ending)):
                    @pl.when(me == ending[e])
                    def _():
                        @pl.when(me == last_group(chip))
                        def _():
                            late[late_place(e)] = ends[last_group(chip)]

                        for k in range(nv):
                            @pl.when(jnp.logical_or(me != last_group(chip), v != k))
                            def _():
                                late_copy(e, k).start()

            @pl.when(jnp.logical_and(u != stop - 1, g != me))
            def _():
                send_end(ways[1], g).start()

            @pl.when(jnp.logical_and(u != stop - 1, g == me))
            def _():
                mine[ways[1]] = ends[g]

    def step(i, carry):
        u = i - places[0] * SKEW
        extra = jnp.where(places[0] == 0, BACK, 0)

        @pl.when(jnp.logical_and(u >= 0, u < units + extra))
        def _():
            @pl.when(jnp.logical_and(places[0] == 0, u > 0))
            def _():
                ship(0, u, held(0, u))

            @pl.when(places[0] > 0)
            def _():
                ship(0, u, received(0, u))

        w = i - places[1] * SKEW

        @pl.when(jnp.logical_and(w >= 0, w < units))
        def _():
            @pl.when(jnp.logical_and(places[1] < n - 1, jnp.logical_or(w < kept, places[1] < n - 2)))
            def _():
                ship(1, w, received(1, w))

            @pl.when(jnp.logical_and(places[1] == n - 1, w < kept))
            def _():
                statistics(w, received(1, w), 0, kept)

            @pl.when(jnp.logical_and(places[1] == n - 2, w >= kept))
            def _():
                total = [a + b for a, b in zip(received(1, w), returned(w + BACK))]
                statistics(w, total, kept, units)

        @pl.when(jnp.logical_and(u >= 0, u < units))
        def _():
            dot(0, u + 1)

        @pl.when(jnp.logical_and(w >= -1, w < jnp.where(places[1] == n - 1, kept, units) - 1))
        def _():
            dot(1, w + 1)

        return carry

    mine_last = jnp.where(places[1] == n - 1, kept, units)
    lax.fori_loop(0, mine_last + places[1] * SKEW, step, 0)

    def merge(tiles):
        top = functools.reduce(jnp.maximum, [t[0:1] for t in tiles])
        weight_sum = sum(t[1:2] * jnp.exp(t[0:1] - top) for t in tiles)
        chosen = sum(t[2:3] for t in tiles)
        return top, weight_sum, chosen

    def c_copy(target):
        return pltpu.make_async_remote_copy(
            src_ref=shared.at[v], dst_ref=shared.at[v], send_sem=c_send, recv_sem=c_recv,
            device_id=(target, me), device_id_type=MESH,
        )

    early = last_group(chip) != me
    at_end = functools.reduce(jnp.logical_or, [me == z for z in ending])
    middle = jnp.logical_or(me == n // 2 - 1, me == n // 2)

    @pl.when(early)
    def _():
        for e in range(2):
            @pl.when(me != finals[e])
            def _():
                send_end(e, me).wait_recv()

        top, weight_sum, chosen = merge([mine[0], mine[1]])
        shared[v] = jnp.concatenate([top, weight_sum, chosen, jnp.zeros((5, 2 * block), jnp.float32)], axis=0)
        for k in range(1, nv):
            c_copy((v + k) % nv).start()

    for _ in range(nv - 1):
        h_copy(v).wait_send()
    def passed(ref, count, sem):
        pltpu.make_async_copy(ref.at[0:count], ref.at[0:count], sem).wait()

    for role, count in ((at_end, len(ending) - 1), (jnp.logical_not(at_end), len(ending))):
        @pl.when(role)
        def _():
            passed(labels, count, l_send)

    def sent(t, count):
        way = ways[t]
        pltpu.make_async_copy(gone.at[way, 0:count], came.at[way, 0:count], q_send.at[way]).wait()
        pltpu.make_async_copy(gone_scale.at[way, 0:count], came_scale.at[way, 0:count], s_send.at[way]).wait()

    for t, role, count in (
        (0, places[0] == 0, units + BACK), (0, places[0] > 0, units),
        (1, places[1] < n - 2, units), (1, places[1] == n - 2, kept),
    ):
        @pl.when(role)
        def _():
            sent(t, count)

    @pl.when(places[1] == n - 1)
    def _():
        passed(ends, groups - 2, e_send)

    for role, count in ((early, nv), (jnp.logical_not(early), nv - 1)):
        @pl.when(jnp.logical_and(role, places[1] >= n - 2))
        def _():
            passed(late, count, t_send)

    for role, count in (
        (jnp.logical_not(middle), nv - 1),
        (jnp.logical_and(middle, early), nv // 2 - 1),
        (jnp.logical_not(early), nv // 2),
    ):
        @pl.when(role)
        def _():
            passed(shared, count, c_recv)

    for role, count in (
        (jnp.logical_and(middle, jnp.logical_or(early, jnp.logical_not(at_end))), late.shape[0]),
        (jnp.logical_and(jnp.logical_not(early), at_end), late.shape[0] - 1),
    ):
        @pl.when(role)
        def _():
            passed(late, count, t_recv)

    top, weight_sum, chosen = merge(
        [shared[k] for k in range(nv)] + [late[k] for k in range(late.shape[0])]
    )
    norm = top + jnp.log(weight_sum)
    for b, line in enumerate((norm, chosen)):
        for a in range(depths):
            out[depths * b + a : depths * b + a + 1, :] = jnp.concatenate(
                [line[:, (s * depths + a) * share : (s * depths + a + 1) * share] for s in range(2)], axis=1
            )

    @pl.when(early)
    def _():
        passed(shared, nv - 1, c_send)


def body(n, nv, hidden, head_weight, targets):
    depths, share, width = hidden.shape
    columns = head_weight.shape[1]
    groups = nv // 2
    assert groups == n and n >= 4 and depths * 2 * share == LANES
    cw = min(512, columns // 2)
    nj = columns // 2 // cw
    units = nv * nj
    block = depths * share
    ring = 16
    while ring < (n - 1) * SKEW + 4:
        ring *= 2
    vmem, anywhere = pl.BlockSpec(memory_space=pltpu.VMEM), pl.BlockSpec(memory_space=pl.ANY)
    dma = pltpu.SemaphoreType.DMA
    result = pl.pallas_call(
        functools.partial(kernel, n, nv, nj, cw, ring),
        out_shape=jax.ShapeDtypeStruct((2 * depths, targets.shape[1]), jnp.float32),
        in_specs=[anywhere, anywhere, anywhere],
        out_specs=vmem,
        scratch_shapes=[
            pltpu.VMEM((groups, 2, depths, share, width), hidden.dtype),
            pltpu.VMEM((2 * nj, width, cw), head_weight.dtype),
            pltpu.VMEM((2, units + BACK, block, cw), jnp.int16),
            pltpu.VMEM((2, units + BACK, block, cw), jnp.int16),
            pltpu.VMEM((2, units + BACK, 1, LANES), jnp.float32),
            pltpu.VMEM((2, units + BACK, 1, LANES), jnp.float32),
            pltpu.VMEM((2, 2, block, cw), jnp.float32),
            pltpu.VMEM((n,) + targets.shape, jnp.int32),
            pltpu.VMEM((2 * block, LANES), jnp.int32),
            pltpu.VMEM((2 * block, LANES), jnp.float32),
            pltpu.VMEM((2 * block, LANES), jnp.float32),
            pltpu.VMEM((2 * block, LANES), jnp.float32),
            pltpu.VMEM((groups, 8, 2 * block), jnp.float32),
            pltpu.VMEM((2, 8, 2 * block), jnp.float32),
            pltpu.VMEM((nv, 8, 2 * block), jnp.float32),
            pltpu.VMEM((2 * nv, 8, 2 * block), jnp.float32),
            dma((2, AHEAD + 1)), dma, dma, dma, dma((nv,)), dma, dma,
            dma((2,)), dma((2, ring)), dma((2,)), dma((2, ring)),
            dma, dma((2,)), dma, dma, dma, dma,
        ],
        compiler_params=pltpu.CompilerParams(
            collective_id=0, has_side_effects=True, vmem_limit_bytes=60 * 1024 * 1024
        ),
    )(hidden, head_weight, targets)
    norm, chosen = result[:depths], result[depths:]
    return norm - chosen, norm * norm


def solution(mesh):
    return jax.shard_map(
        functools.partial(body, mesh.shape["hid"], mesh.shape["vocab"]),
        mesh=mesh,
        in_specs=(P(None, "vocab", "hid"), P("hid", "vocab"), P(None, "hid")),
        out_specs=(P(None, "hid"), P(None, "hid")),
        check_vma=False,
    )
```

```python
import functools

import jax
import jax.numpy as jnp
from jax import lax
from jax.experimental import pallas as pl
from jax.experimental.pallas import tpu as pltpu
from jax.sharding import PartitionSpec as P

MESH = pl.DeviceIdType.MESH
LANES = 128
SKEW = 3
AHEAD = 3
BACK = 3
LOWEST = -3.0e38
TOP = 32767.0


def kernel(
    n, nv, nj, cw, ring,
    hidden, weight, targets,
    out,
    rows, wbuf, came, gone, came_scale, gone_scale, part,
    labels, label_tile, peak, mass, pick, ends, mine, shared, late,
    w_sem, own_sem, label_sem, h_send, h_recv, l_send, l_recv,
    q_send, q_recv, s_send, s_recv, e_send, e_recv, c_send, c_recv, t_send, t_recv,
):
    v, me = lax.axis_index("vocab"), lax.axis_index("hid")
    groups = nv // 2
    chip, parity = v // 2, v % 2
    depths, share, width = hidden.shape
    block = depths * share
    half = nj * cw
    span = 2 * nj
    units = nv * nj
    columns = [slice(c * LANES, (c + 1) * LANES) for c in range(cw // LANES)]
    low = me < n // 2
    ways = (jnp.where(low, 0, 1), jnp.where(low, 1, 0))
    near = jnp.where(low, me, n - 1 - me)
    places = (near, n - 1 - near)
    nexts = (jnp.where(low, me + 1, me - 1), jnp.where(low, me - 1, me + 1))

    kept = units - BACK
    ending = (0, 1, n - 2, n - 1)

    def last_group(c):
        return n // 2 - 1 + c % 2

    def w_copy(t, j):
        return pltpu.make_async_copy(
            weight.at[:, pl.ds(pl.multiple_of(ways[t] * half + j * cw, cw), cw)],
            wbuf.at[ways[t] * nj + j],
            w_sem.at[t, j % (AHEAD + 1)],
        )

    own = pltpu.make_async_copy(hidden, rows.at[chip, parity], own_sem)
    own.start()
    w_copy(0, 0).start()
    row = lax.broadcasted_iota(jnp.int32, (8, 2 * block), 0)
    neutral = jnp.where(row == 0, LOWEST, 0.0)
    for k in range(nv):
        shared[k] = neutral
    for k in range(late.shape[0]):
        late[k] = neutral

    barrier = pltpu.get_barrier_semaphore()
    for k in range(1, nv):
        pl.semaphore_signal(barrier, inc=1, device_id=((v + k) % nv, me), device_id_type=MESH)
    for k in range(1, n):
        pl.semaphore_signal(barrier, inc=1, device_id=(v, (me + k) % n), device_id_type=MESH)

    def h_copy(target):
        return pltpu.make_async_remote_copy(
            src_ref=hidden, dst_ref=rows.at[chip, parity], send_sem=h_send, recv_sem=h_recv.at[v],
            device_id=(target, me), device_id_type=MESH,
        )

    def h_arrival(g, side):
        return pltpu.make_async_remote_copy(
            src_ref=hidden, dst_ref=rows.at[g, side], send_sem=h_send, recv_sem=h_recv.at[2 * g + side],
            device_id=(v, me), device_id_type=MESH,
        )

    def small_dot(t, u):
        j = u % nj
        a = rows[chip, (v + u // nj) % 2].reshape(block, width)
        part[t, u % 2] = jnp.dot(a, wbuf[ways[t] * nj + j], preferred_element_type=jnp.float32)

    def group_of(u):
        turn = u // span
        natural, final = (chip + turn) % groups, last_group(chip)
        other = jnp.where(natural == final, (chip + groups - 1) % groups, natural)
        return jnp.where(turn == groups - 1, final, other)

    def big_dot(t, g, chunk):
        a = rows[g].reshape(2 * block, width)
        y = jnp.dot(a, wbuf[chunk], preferred_element_type=jnp.float32)
        part[t] = y.reshape(2, block, cw)

    def dot(t, u):
        @pl.when(u < span)
        def _():
            @pl.when(u < nj)
            def _():
                @pl.when(u + AHEAD - 1 < nj)
                def _():
                    w_copy(t, u + AHEAD - 1).start()

                w_copy(t, u).wait()

            if t == 0:
                @pl.when(u == nj)
                def _():
                    h_arrival(chip, 1 - parity).wait_recv()

            small_dot(t, u)

        @pl.when(jnp.logical_and(jnp.logical_and(u >= span, u < units), u % 2 == 0))
        def _():
            g = group_of(u)
            if t == 0:
                @pl.when(u % span == 0)
                def _():
                    for side in range(2):
                        h_arrival(g, side).wait_recv()

            big_dot(t, g, ways[t] * nj + (u % span) // 2)

        if t == 0:
            @pl.when(u >= units)
            def _():
                back = u - BACK
                a = rows[last_group(chip), back % 2].reshape(block, width)
                chunk = ways[1] * nj + (back % span) // 2
                part[0, u % 2] = jnp.dot(a, wbuf[chunk], preferred_element_type=jnp.float32)

    finals = (n - 1, 0)

    def l_copy(e):
        return pltpu.make_async_remote_copy(
            src_ref=targets, dst_ref=labels.at[me], send_sem=l_send, recv_sem=l_recv,
            device_id=(v, ending[e]), device_id_type=MESH,
        )

    def message(t, u, target):
        way = ways[t]
        data = pltpu.make_async_remote_copy(
            src_ref=gone.at[way, u], dst_ref=came.at[way, u],
            send_sem=q_send.at[way], recv_sem=q_recv.at[way, u % ring],
            device_id=(v, target), device_id_type=MESH,
        )
        scale = pltpu.make_async_remote_copy(
            src_ref=gone_scale.at[way, u], dst_ref=came_scale.at[way, u],
            send_sem=s_send.at[way], recv_sem=s_recv.at[way, u % ring],
            device_id=(v, target), device_id_type=MESH,
        )
        return scale, data

    def send_end(e, g):
        return pltpu.make_async_remote_copy(
            src_ref=ends.at[g], dst_ref=mine.at[e], send_sem=e_send, recv_sem=e_recv.at[e],
            device_id=(v, g), device_id_type=MESH,
        )

    def held(t, u):
        return [part[t, u % 2, :, c] for c in columns]

    def received(t, u):
        for copy in message(t, u, me):
            copy.wait_recv()
        scale = came_scale[ways[t], u]
        return [
            part[t, u % 2, :, c] + came[ways[t], u, :, c].astype(jnp.int32).astype(jnp.float32) * scale
            for c in columns
        ]

    def returned(u):
        for copy in message(0, u, me):
            copy.wait_recv()
        scale = came_scale[ways[0], u]
        return [came[ways[0], u, :, c].astype(jnp.int32).astype(jnp.float32) * scale for c in columns]

    def late_place(e):
        return (chip // 2 * 2 + parity) * len(ending) + e

    def late_copy(e, target):
        return pltpu.make_async_remote_copy(
            src_ref=ends.at[last_group(chip)], dst_ref=late.at[late_place(e)], send_sem=t_send, recv_sem=t_recv,
            device_id=(target, last_group(chip)), device_id_type=MESH,
        )

    def prepare(t, u, pieces):
        largest = functools.reduce(jnp.maximum, [jnp.abs(piece) for piece in pieces])
        largest = jnp.maximum(jnp.max(largest, axis=0, keepdims=True), 1e-30)
        gone_scale[ways[t], u] = largest * (1.0 / TOP)
        up = TOP / largest
        for c, piece in zip(columns, pieces):
            gone[ways[t], u, :, c] = jnp.round(piece * up).astype(jnp.int32).astype(jnp.int16)

    def launch(t, u):
        for copy in message(t, u, nexts[t]):
            copy.start()

    def ship(t, u, pieces):
        prepare(t, u, pieces)
        launch(t, u)

    own.wait()
    w_copy(0, 0).wait()
    for j in range(1, AHEAD):
        w_copy(0, j).start()
    for j in range(AHEAD - 1):
        w_copy(1, j).start()

    small_dot(0, 0)

    @pl.when(places[0] == 0)
    def _():
        prepare(0, 0, held(0, 0))

    pl.semaphore_wait(barrier, nv - 1 + n - 1)

    @pl.when(places[0] == 0)
    def _():
        launch(0, 0)

    peers = [2 * chip + 1 - parity]
    for back in range(1, groups):
        other = (chip - back + groups) % groups
        peers += [2 * other + parity, 2 * other + 1 - parity]
    for target in peers:
        h_copy(target).start()

    for e in range(len(ending)):
        @pl.when(me != ending[e])
        def _():
            l_copy(e).start()

    own_labels = pltpu.make_async_copy(targets, labels.at[me], label_sem)
    own_labels.start()

    def order(line):
        return jnp.concatenate(
            [line[a : a + 1, s * share : (s + 1) * share] for s in range(2) for a in range(depths)], axis=1
        )

    def statistics(u, pieces, start, stop):
        g, r = group_of(u), u % span

        @pl.when(u == start)
        def _():
            pltpu.make_async_copy(labels.at[0 : n - 1], labels.at[1:n], l_recv).wait()
            pltpu.make_async_copy(targets, labels.at[me], label_sem).wait()

        @pl.when(jnp.logical_or(r == 0, u == start))
        def _():
            label_tile[...] = jnp.transpose(jnp.broadcast_to(order(labels[g]), (LANES, 2 * block)))
            peak[...] = jnp.full_like(peak, LOWEST)
            mass[...] = jnp.zeros_like(mass)
            pick[...] = jnp.zeros_like(pick)

        first_group = u < span
        side = jnp.where(first_group, (v + u // nj) % 2, r % 2)
        j = jnp.where(first_group, u % nj, r // 2)
        here = pl.ds(pl.multiple_of(side * block, block), block)
        old = peak[here, :]
        new = functools.reduce(jnp.maximum, pieces, old)
        peak[here, :] = new
        mass[here, :] = mass[here, :] * jnp.exp(old - new) + sum(jnp.exp(piece - new) for piece in pieces)
        offset = label_tile[here, :] - (v * (2 * half) + ways[1] * half + j * cw)
        lane = lax.broadcasted_iota(jnp.int32, (block, LANES), 1)
        found = pick[here, :]
        for c, piece in enumerate(pieces):
            found = found + jnp.where(offset == lane + c * LANES, piece, 0.0)
        pick[here, :] = found

        @pl.when(jnp.logical_or(r == span - 1, u == stop - 1))
        def _():
            tall = jnp.transpose(peak[...])
            top = jnp.max(tall, axis=0, keepdims=True)
            weight_sum = jnp.sum(jnp.transpose(mass[...]) * jnp.exp(tall - top), axis=0, keepdims=True)
            chosen = jnp.sum(jnp.transpose(pick[...]), axis=0, keepdims=True)
            ends[g] = jnp.concatenate(
                [top, weight_sum, chosen, jnp.zeros((5, 2 * block), jnp.float32)], axis=0
            )

            @pl.when(u == stop - 1)
            def _():
                for e in range(len(ending)):
                    @pl.when(me == ending[e])
                    def _():
                        @pl.when(me == last_group(chip))
                        def _():
                            late[late_place(e)] = ends[last_group(chip)]

                        for k in range(nv):
                            @pl.when(jnp.logical_or(me != last_group(chip), v != k))
                            def _():
                                late_copy(e, k).start()

            @pl.when(jnp.logical_and(u != stop - 1, g != me))
            def _():
                send_end(ways[1], g).start()

            @pl.when(jnp.logical_and(u != stop - 1, g == me))
            def _():
                mine[ways[1]] = ends[g]

    def merge(tiles):
        top = functools.reduce(jnp.maximum, [t[0:1] for t in tiles])
        weight_sum = sum(t[1:2] * jnp.exp(t[0:1] - top) for t in tiles)
        chosen = sum(t[2:3] for t in tiles)
        return top, weight_sum, chosen

    def c_copy(target):
        return pltpu.make_async_remote_copy(
            src_ref=shared.at[v], dst_ref=shared.at[v], send_sem=c_send, recv_sem=c_recv,
            device_id=(target, me), device_id_type=MESH,
        )

    early = last_group(chip) != me
    at_end = functools.reduce(jnp.logical_or, [me == z for z in ending])
    middle = jnp.logical_or(me == n // 2 - 1, me == n // 2)

    def exchange():
        for e in range(2):
            @pl.when(me != finals[e])
            def _():
                send_end(e, me).wait_recv()

        top, weight_sum, chosen = merge([mine[0], mine[1]])
        shared[v] = jnp.concatenate([top, weight_sum, chosen, jnp.zeros((5, 2 * block), jnp.float32)], axis=0)
        for k in range(1, nv):
            c_copy((v + k) % nv).start()

    def passed(ref, count, sem):
        pltpu.make_async_copy(ref.at[0:count], ref.at[0:count], sem).wait()

    def step(i, carry):
        u = i - places[0] * SKEW
        extra = jnp.where(places[0] == 0, BACK, 0)

        @pl.when(jnp.logical_and(u >= 0, u < units + extra))
        def _():
            @pl.when(jnp.logical_and(places[0] == 0, u > 0))
            def _():
                ship(0, u, held(0, u))

            @pl.when(places[0] > 0)
            def _():
                ship(0, u, received(0, u))

        w = i - places[1] * SKEW

        @pl.when(jnp.logical_and(w >= 0, w < units))
        def _():
            @pl.when(jnp.logical_and(places[1] < n - 1, jnp.logical_or(w < kept, places[1] < n - 2)))
            def _():
                ship(1, w, received(1, w))

            @pl.when(jnp.logical_and(places[1] == n - 1, w < kept))
            def _():
                statistics(w, received(1, w), 0, kept)

            @pl.when(jnp.logical_and(places[1] == n - 2, w >= kept))
            def _():
                total = [a + b for a, b in zip(received(1, w), returned(w + BACK))]
                statistics(w, total, kept, units)

        @pl.when(jnp.logical_and(u >= 0, u < units + extra - 1))
        def _():
            dot(0, u + 1)

        @pl.when(jnp.logical_and(w == units - nj, early))
        def _():
            exchange()

        @pl.when(jnp.logical_and(w >= -1, w < jnp.where(places[1] == n - 1, kept, units) - 1))
        def _():
            dot(1, w + 1)

        return carry

    mine_last = jnp.where(places[1] == n - 1, kept, units)
    lax.fori_loop(0, mine_last + places[1] * SKEW, step, 0)

    for role, count in (
        (jnp.logical_not(middle), nv - 1),
        (jnp.logical_and(middle, early), nv // 2 - 1),
        (jnp.logical_not(early), nv // 2),
    ):
        @pl.when(role)
        def _():
            passed(shared, count, c_recv)

    for role, count in (
        (jnp.logical_and(middle, jnp.logical_or(early, jnp.logical_not(at_end))), late.shape[0]),
        (jnp.logical_and(jnp.logical_not(early), at_end), late.shape[0] - 1),
    ):
        @pl.when(role)
        def _():
            passed(late, count, t_recv)

    def finish(tiles):
        top, weight_sum, chosen = merge(tiles)
        norm = top + jnp.log(weight_sum)
        for b, line in enumerate((norm, chosen)):
            for a in range(depths):
                out[depths * b + a : depths * b + a + 1, :] = jnp.concatenate(
                    [line[:, (s * depths + a) * share : (s * depths + a + 1) * share] for s in range(2)], axis=1
                )

    @pl.when(middle)
    def _():
        finish([shared[k] for k in range(nv)] + [late[k] for k in range(late.shape[0])])

    @pl.when(jnp.logical_not(middle))
    def _():
        finish([shared[k] for k in range(nv)])

    for _ in range(nv - 1):
        h_copy(v).wait_send()
    for role, count in ((at_end, len(ending) - 1), (jnp.logical_not(at_end), len(ending))):
        @pl.when(role)
        def _():
            passed(labels, count, l_send)

    def sent(t, count):
        way = ways[t]
        pltpu.make_async_copy(gone.at[way, 0:count], came.at[way, 0:count], q_send.at[way]).wait()
        pltpu.make_async_copy(gone_scale.at[way, 0:count], came_scale.at[way, 0:count], s_send.at[way]).wait()

    for t, role, count in (
        (0, places[0] == 0, units + BACK), (0, places[0] > 0, units),
        (1, places[1] < n - 2, units), (1, places[1] == n - 2, kept),
    ):
        @pl.when(role)
        def _():
            sent(t, count)

    @pl.when(places[1] == n - 1)
    def _():
        passed(ends, groups - 2, e_send)

    for role, count in ((early, nv), (jnp.logical_not(early), nv - 1)):
        @pl.when(jnp.logical_and(role, places[1] >= n - 2))
        def _():
            passed(late, count, t_send)

    @pl.when(early)
    def _():
        passed(shared, nv - 1, c_send)


def body(n, nv, hidden, head_weight, targets):
    depths, share, width = hidden.shape
    columns = head_weight.shape[1]
    groups = nv // 2
    assert groups == n and n >= 4 and depths * 2 * share == LANES
    cw = min(512, columns // 2)
    nj = columns // 2 // cw
    units = nv * nj
    block = depths * share
    ring = 16
    while ring < (n - 1) * SKEW + 4:
        ring *= 2
    vmem, anywhere = pl.BlockSpec(memory_space=pltpu.VMEM), pl.BlockSpec(memory_space=pl.ANY)
    dma = pltpu.SemaphoreType.DMA
    result = pl.pallas_call(
        functools.partial(kernel, n, nv, nj, cw, ring),
        out_shape=jax.ShapeDtypeStruct((2 * depths, targets.shape[1]), jnp.float32),
        in_specs=[anywhere, anywhere, anywhere],
        out_specs=vmem,
        scratch_shapes=[
            pltpu.VMEM((groups, 2, depths, share, width), hidden.dtype),
            pltpu.VMEM((2 * nj, width, cw), head_weight.dtype),
            pltpu.VMEM((2, units + BACK, block, cw), jnp.int16),
            pltpu.VMEM((2, units + BACK, block, cw), jnp.int16),
            pltpu.VMEM((2, units + BACK, 1, LANES), jnp.float32),
            pltpu.VMEM((2, units + BACK, 1, LANES), jnp.float32),
            pltpu.VMEM((2, 2, block, cw), jnp.float32),
            pltpu.VMEM((n,) + targets.shape, jnp.int32),
            pltpu.VMEM((2 * block, LANES), jnp.int32),
            pltpu.VMEM((2 * block, LANES), jnp.float32),
            pltpu.VMEM((2 * block, LANES), jnp.float32),
            pltpu.VMEM((2 * block, LANES), jnp.float32),
            pltpu.VMEM((groups, 8, 2 * block), jnp.float32),
            pltpu.VMEM((2, 8, 2 * block), jnp.float32),
            pltpu.VMEM((nv, 8, 2 * block), jnp.float32),
            pltpu.VMEM((2 * nv, 8, 2 * block), jnp.float32),
            dma((2, AHEAD + 1)), dma, dma, dma, dma((nv,)), dma, dma,
            dma((2,)), dma((2, ring)), dma((2,)), dma((2, ring)),
            dma, dma((2,)), dma, dma, dma, dma,
        ],
        compiler_params=pltpu.CompilerParams(
            collective_id=0, has_side_effects=True, vmem_limit_bytes=60 * 1024 * 1024
        ),
    )(hidden, head_weight, targets)
    norm, chosen = result[:depths], result[depths:]
    return norm - chosen, norm * norm


def solution(mesh):
    return jax.shard_map(
        functools.partial(body, mesh.shape["hid"], mesh.shape["vocab"]),
        mesh=mesh,
        in_specs=(P(None, "vocab", "hid"), P("hid", "vocab"), P(None, "hid")),
        out_specs=(P(None, "hid"), P(None, "hid")),
        check_vma=False,
    )
```

```python
import functools

import jax
import jax.numpy as jnp
from jax import lax
from jax.experimental import pallas as pl
from jax.experimental.pallas import tpu as pltpu
from jax.sharding import PartitionSpec as P

MESH = pl.DeviceIdType.MESH
LANES = 128
SKEW = 3
AHEAD = 3
BACK = 3
LOWEST = -3.0e38
TOP = 32767.0


def kernel(
    n, nv, nj, cw, ring,
    hidden, weight, targets,
    out,
    rows, wbuf, came, gone, came_scale, gone_scale, part,
    labels, label_tile, peak, mass, pick, ends, mine, shared, late,
    w_sem, own_sem, label_sem, h_send, h_recv, l_send, l_recv,
    q_send, q_recv, s_send, s_recv, e_send, e_recv, c_send, c_recv, t_send, t_recv,
):
    v, me = lax.axis_index("vocab"), lax.axis_index("hid")
    groups = nv // 2
    chip, parity = v // 2, v % 2
    depths, share, width = hidden.shape
    block = depths * share
    half = nj * cw
    span = 2 * nj
    units = nv * nj
    columns = [slice(c * LANES, (c + 1) * LANES) for c in range(cw // LANES)]
    low = me < n // 2
    ways = (jnp.where(low, 0, 1), jnp.where(low, 1, 0))
    near = jnp.where(low, me, n - 1 - me)
    places = (near, n - 1 - near)
    nexts = (jnp.where(low, me + 1, me - 1), jnp.where(low, me - 1, me + 1))

    kept = units - BACK
    ending = (0, 1, n - 2, n - 1)

    def last_group(c):
        return n // 2 - 1 + c % 2

    def w_copy(t, j):
        return pltpu.make_async_copy(
            weight.at[:, pl.ds(pl.multiple_of(ways[t] * half + j * cw, cw), cw)],
            wbuf.at[ways[t] * nj + j],
            w_sem.at[t, j % (AHEAD + 1)],
        )

    own = pltpu.make_async_copy(hidden, rows.at[chip, parity], own_sem)
    own.start()
    w_copy(0, 0).start()
    row = lax.broadcasted_iota(jnp.int32, (4, 2 * block), 0)
    neutral = jnp.where(row == 0, LOWEST, 0.0)
    for k in range(nv):
        shared[k] = neutral
    for k in range(late.shape[0]):
        late[k] = neutral

    barrier = pltpu.get_barrier_semaphore()
    for k in range(1, nv):
        pl.semaphore_signal(barrier, inc=1, device_id=((v + k) % nv, me), device_id_type=MESH)
    for k in range(1, n):
        pl.semaphore_signal(barrier, inc=1, device_id=(v, (me + k) % n), device_id_type=MESH)

    def h_copy(target):
        return pltpu.make_async_remote_copy(
            src_ref=hidden, dst_ref=rows.at[chip, parity], send_sem=h_send, recv_sem=h_recv.at[v],
            device_id=(target, me), device_id_type=MESH,
        )

    def h_arrival(g, side):
        return pltpu.make_async_remote_copy(
            src_ref=hidden, dst_ref=rows.at[g, side], send_sem=h_send, recv_sem=h_recv.at[2 * g + side],
            device_id=(v, me), device_id_type=MESH,
        )

    def small_dot(t, u):
        j = u % nj
        a = rows[chip, (v + u // nj) % 2].reshape(block, width)
        part[t, u % 2] = jnp.dot(a, wbuf[ways[t] * nj + j], preferred_element_type=jnp.float32)

    def group_of(u):
        turn = u // span
        natural, final = (chip + turn) % groups, last_group(chip)
        other = jnp.where(natural == final, (chip + groups - 1) % groups, natural)
        return jnp.where(turn == groups - 1, final, other)

    def big_dot(t, g, chunk):
        a = rows[g].reshape(2 * block, width)
        y = jnp.dot(a, wbuf[chunk], preferred_element_type=jnp.float32)
        part[t] = y.reshape(2, block, cw)

    def dot(t, u):
        @pl.when(u < span)
        def _():
            @pl.when(u < nj)
            def _():
                @pl.when(u + AHEAD - 1 < nj)
                def _():
                    w_copy(t, u + AHEAD - 1).start()

                w_copy(t, u).wait()

            if t == 0:
                @pl.when(u == nj)
                def _():
                    h_arrival(chip, 1 - parity).wait_recv()

            small_dot(t, u)

        @pl.when(jnp.logical_and(jnp.logical_and(u >= span, u < units), u % 2 == 0))
        def _():
            g = group_of(u)
            if t == 0:
                @pl.when(u % span == 0)
                def _():
                    for side in range(2):
                        h_arrival(g, side).wait_recv()

            big_dot(t, g, ways[t] * nj + (u % span) // 2)

        if t == 0:
            @pl.when(u >= units)
            def _():
                back = u - BACK
                a = rows[last_group(chip), back % 2].reshape(block, width)
                chunk = ways[1] * nj + (back % span) // 2
                part[0, u % 2] = jnp.dot(a, wbuf[chunk], preferred_element_type=jnp.float32)

    finals = (n - 1, 0)

    def l_copy(e):
        return pltpu.make_async_remote_copy(
            src_ref=targets, dst_ref=labels.at[me], send_sem=l_send, recv_sem=l_recv,
            device_id=(v, ending[e]), device_id_type=MESH,
        )

    def message(t, u, target):
        way = ways[t]
        data = pltpu.make_async_remote_copy(
            src_ref=gone.at[way, u], dst_ref=came.at[way, u],
            send_sem=q_send.at[way], recv_sem=q_recv.at[way, u % ring],
            device_id=(v, target), device_id_type=MESH,
        )
        scale = pltpu.make_async_remote_copy(
            src_ref=gone_scale.at[way, u], dst_ref=came_scale.at[way, u],
            send_sem=s_send.at[way], recv_sem=s_recv.at[way, u % ring],
            device_id=(v, target), device_id_type=MESH,
        )
        return scale, data

    def send_end(e, g):
        return pltpu.make_async_remote_copy(
            src_ref=ends.at[g], dst_ref=mine.at[e], send_sem=e_send, recv_sem=e_recv.at[e],
            device_id=(v, g), device_id_type=MESH,
        )

    def held(t, u):
        return [part[t, u % 2, :, c] for c in columns]

    def received(t, u):
        for copy in message(t, u, me):
            copy.wait_recv()
        scale = came_scale[ways[t], u]
        return [
            part[t, u % 2, :, c] + came[ways[t], u, :, c].astype(jnp.int32).astype(jnp.float32) * scale
            for c in columns
        ]

    def returned(u):
        for copy in message(0, u, me):
            copy.wait_recv()
        scale = came_scale[ways[0], u]
        return [came[ways[0], u, :, c].astype(jnp.int32).astype(jnp.float32) * scale for c in columns]

    def late_place(e):
        return (chip // 2 * 2 + parity) * len(ending) + e

    def late_copy(e, target):
        return pltpu.make_async_remote_copy(
            src_ref=ends.at[last_group(chip)], dst_ref=late.at[late_place(e)], send_sem=t_send, recv_sem=t_recv,
            device_id=(target, last_group(chip)), device_id_type=MESH,
        )

    def prepare(t, u, pieces):
        largest = functools.reduce(jnp.maximum, [jnp.abs(piece) for piece in pieces])
        largest = jnp.maximum(jnp.max(largest, axis=0, keepdims=True), 1e-30)
        gone_scale[ways[t], u] = largest * (1.0 / TOP)
        up = TOP / largest
        for c, piece in zip(columns, pieces):
            gone[ways[t], u, :, c] = jnp.round(piece * up).astype(jnp.int32).astype(jnp.int16)

    def launch(t, u):
        for copy in message(t, u, nexts[t]):
            copy.start()

    def ship(t, u, pieces):
        prepare(t, u, pieces)
        launch(t, u)

    own.wait()
    w_copy(0, 0).wait()
    for j in range(1, AHEAD):
        w_copy(0, j).start()
    for j in range(AHEAD - 1):
        w_copy(1, j).start()

    small_dot(0, 0)

    @pl.when(places[0] == 0)
    def _():
        prepare(0, 0, held(0, 0))

    pl.semaphore_wait(barrier, nv - 1 + n - 1)

    @pl.when(places[0] == 0)
    def _():
        launch(0, 0)

    peers = [2 * chip + 1 - parity]
    for back in range(1, groups):
        other = (chip - back + groups) % groups
        peers += [2 * other + parity, 2 * other + 1 - parity]
    for target in peers:
        h_copy(target).start()

    for e in range(len(ending)):
        @pl.when(me != ending[e])
        def _():
            l_copy(e).start()

    own_labels = pltpu.make_async_copy(targets, labels.at[me], label_sem)
    own_labels.start()

    def order(line):
        return jnp.concatenate(
            [line[a : a + 1, s * share : (s + 1) * share] for s in range(2) for a in range(depths)], axis=1
        )

    def statistics(u, pieces, start, stop):
        g, r = group_of(u), u % span

        @pl.when(u == start)
        def _():
            pltpu.make_async_copy(labels.at[0 : n - 1], labels.at[1:n], l_recv).wait()
            pltpu.make_async_copy(targets, labels.at[me], label_sem).wait()

        @pl.when(jnp.logical_or(r == 0, u == start))
        def _():
            label_tile[...] = jnp.transpose(jnp.broadcast_to(order(labels[g]), (LANES, 2 * block)))
            peak[...] = jnp.full_like(peak, LOWEST)
            mass[...] = jnp.zeros_like(mass)
            pick[...] = jnp.zeros_like(pick)

        first_group = u < span
        side = jnp.where(first_group, (v + u // nj) % 2, r % 2)
        j = jnp.where(first_group, u % nj, r // 2)
        here = pl.ds(pl.multiple_of(side * block, block), block)
        old = peak[here, :]
        new = functools.reduce(jnp.maximum, pieces, old)
        peak[here, :] = new
        mass[here, :] = mass[here, :] * jnp.exp(old - new) + sum(jnp.exp(piece - new) for piece in pieces)
        offset = label_tile[here, :] - (v * (2 * half) + ways[1] * half + j * cw)
        lane = lax.broadcasted_iota(jnp.int32, (block, LANES), 1)
        found = pick[here, :]
        for c, piece in enumerate(pieces):
            found = found + jnp.where(offset == lane + c * LANES, piece, 0.0)
        pick[here, :] = found

        @pl.when(jnp.logical_or(r == span - 1, u == stop - 1))
        def _():
            tall = jnp.transpose(peak[...])
            top = jnp.max(tall, axis=0, keepdims=True)
            weight_sum = jnp.sum(jnp.transpose(mass[...]) * jnp.exp(tall - top), axis=0, keepdims=True)
            chosen = jnp.sum(jnp.transpose(pick[...]), axis=0, keepdims=True)
            ends[g] = jnp.concatenate(
                [top, weight_sum, chosen, jnp.zeros((1, 2 * block), jnp.float32)], axis=0
            )

            @pl.when(u == stop - 1)
            def _():
                for e in range(len(ending)):
                    @pl.when(me == ending[e])
                    def _():
                        @pl.when(me == last_group(chip))
                        def _():
                            late[late_place(e)] = ends[last_group(chip)]

                        for k in range(nv):
                            @pl.when(jnp.logical_or(me != last_group(chip), v != k))
                            def _():
                                late_copy(e, k).start()

            @pl.when(jnp.logical_and(u != stop - 1, g != me))
            def _():
                send_end(ways[1], g).start()

            @pl.when(jnp.logical_and(u != stop - 1, g == me))
            def _():
                mine[ways[1]] = ends[g]

    def merge(tiles):
        def pairwise(join, terms):
            while len(terms) > 1:
                terms = [join(*terms[k : k + 2]) if k + 1 < len(terms) else terms[k] for k in range(0, len(terms), 2)]
            return terms[0]

        top = pairwise(jnp.maximum, [t[0:1] for t in tiles])
        weight_sum = pairwise(jnp.add, [t[1:2] * jnp.exp(t[0:1] - top) for t in tiles])
        chosen = pairwise(jnp.add, [t[2:3] for t in tiles])
        return top, weight_sum, chosen

    def c_copy(target):
        return pltpu.make_async_remote_copy(
            src_ref=shared.at[v], dst_ref=shared.at[v], send_sem=c_send, recv_sem=c_recv,
            device_id=(target, me), device_id_type=MESH,
        )

    early = last_group(chip) != me
    at_end = functools.reduce(jnp.logical_or, [me == z for z in ending])
    middle = jnp.logical_or(me == n // 2 - 1, me == n // 2)

    def exchange():
        for e in range(2):
            @pl.when(me != finals[e])
            def _():
                send_end(e, me).wait_recv()

        top, weight_sum, chosen = merge([mine[0], mine[1]])
        shared[v] = jnp.concatenate([top, weight_sum, chosen, jnp.zeros((1, 2 * block), jnp.float32)], axis=0)
        for k in range(1, nv):
            c_copy((v + k) % nv).start()

    def passed(ref, count, sem):
        pltpu.make_async_copy(ref.at[0:count], ref.at[0:count], sem).wait()

    def step(i, carry):
        u = i - places[0] * SKEW
        extra = jnp.where(places[0] == 0, BACK, 0)

        @pl.when(jnp.logical_and(u >= 0, u < units + extra))
        def _():
            @pl.when(jnp.logical_and(places[0] == 0, u > 0))
            def _():
                ship(0, u, held(0, u))

            @pl.when(places[0] > 0)
            def _():
                ship(0, u, received(0, u))

        w = i - places[1] * SKEW

        @pl.when(jnp.logical_and(w >= 0, w < units))
        def _():
            @pl.when(jnp.logical_and(places[1] < n - 1, jnp.logical_or(w < kept, places[1] < n - 2)))
            def _():
                ship(1, w, received(1, w))

            @pl.when(jnp.logical_and(places[1] == n - 1, w < kept))
            def _():
                statistics(w, received(1, w), 0, kept)

            @pl.when(jnp.logical_and(places[1] == n - 2, w >= kept))
            def _():
                total = [a + b for a, b in zip(received(1, w), returned(w + BACK))]
                statistics(w, total, kept, units)

        @pl.when(jnp.logical_and(u >= 0, u < units + extra - 1))
        def _():
            dot(0, u + 1)

        @pl.when(jnp.logical_and(w == units - nj, early))
        def _():
            exchange()

        @pl.when(jnp.logical_and(w >= -1, w < jnp.where(places[1] == n - 1, kept, units) - 1))
        def _():
            dot(1, w + 1)

        return carry

    mine_last = jnp.where(places[1] == n - 1, kept, units)
    lax.fori_loop(0, mine_last + places[1] * SKEW, step, 0)

    for role, count in (
        (jnp.logical_not(middle), nv - 1),
        (jnp.logical_and(middle, early), nv // 2 - 1),
        (jnp.logical_not(early), nv // 2),
    ):
        @pl.when(role)
        def _():
            passed(shared, count, c_recv)

    for role, count in (
        (jnp.logical_and(middle, jnp.logical_or(early, jnp.logical_not(at_end))), late.shape[0]),
        (jnp.logical_and(jnp.logical_not(early), at_end), late.shape[0] - 1),
    ):
        @pl.when(role)
        def _():
            passed(late, count, t_recv)

    def finish(tiles):
        top, weight_sum, chosen = merge(tiles)
        norm = top + jnp.log(weight_sum)
        for b, line in enumerate((norm, chosen)):
            for a in range(depths):
                out[depths * b + a : depths * b + a + 1, :] = jnp.concatenate(
                    [line[:, (s * depths + a) * share : (s * depths + a + 1) * share] for s in range(2)], axis=1
                )

    @pl.when(middle)
    def _():
        finish([shared[k] for k in range(nv)] + [late[k] for k in range(late.shape[0])])

    @pl.when(jnp.logical_not(middle))
    def _():
        finish([shared[k] for k in range(nv)])

    for _ in range(nv - 1):
        h_copy(v).wait_send()
    for role, count in ((at_end, len(ending) - 1), (jnp.logical_not(at_end), len(ending))):
        @pl.when(role)
        def _():
            passed(labels, count, l_send)

    def sent(t, count):
        way = ways[t]
        pltpu.make_async_copy(gone.at[way, 0:count], came.at[way, 0:count], q_send.at[way]).wait()
        pltpu.make_async_copy(gone_scale.at[way, 0:count], came_scale.at[way, 0:count], s_send.at[way]).wait()

    for t, role, count in (
        (0, places[0] == 0, units + BACK), (0, places[0] > 0, units),
        (1, places[1] < n - 2, units), (1, places[1] == n - 2, kept),
    ):
        @pl.when(role)
        def _():
            sent(t, count)

    @pl.when(places[1] == n - 1)
    def _():
        passed(ends, groups - 2, e_send)

    for role, count in ((early, nv), (jnp.logical_not(early), nv - 1)):
        @pl.when(jnp.logical_and(role, places[1] >= n - 2))
        def _():
            passed(late, count, t_send)

    @pl.when(early)
    def _():
        passed(shared, nv - 1, c_send)


def body(n, nv, hidden, head_weight, targets):
    depths, share, width = hidden.shape
    columns = head_weight.shape[1]
    groups = nv // 2
    assert groups == n and n >= 4 and depths * 2 * share == LANES
    cw = min(512, columns // 2)
    nj = columns // 2 // cw
    units = nv * nj
    block = depths * share
    ring = 16
    while ring < (n - 1) * SKEW + 4:
        ring *= 2
    vmem, anywhere = pl.BlockSpec(memory_space=pltpu.VMEM), pl.BlockSpec(memory_space=pl.ANY)
    dma = pltpu.SemaphoreType.DMA
    result = pl.pallas_call(
        functools.partial(kernel, n, nv, nj, cw, ring),
        out_shape=jax.ShapeDtypeStruct((2 * depths, targets.shape[1]), jnp.float32),
        in_specs=[anywhere, anywhere, anywhere],
        out_specs=vmem,
        scratch_shapes=[
            pltpu.VMEM((groups, 2, depths, share, width), hidden.dtype),
            pltpu.VMEM((2 * nj, width, cw), head_weight.dtype),
            pltpu.VMEM((2, units + BACK, block, cw), jnp.int16),
            pltpu.VMEM((2, units + BACK, block, cw), jnp.int16),
            pltpu.VMEM((2, units + BACK, 1, LANES), jnp.float32),
            pltpu.VMEM((2, units + BACK, 1, LANES), jnp.float32),
            pltpu.VMEM((2, 2, block, cw), jnp.float32),
            pltpu.VMEM((n,) + targets.shape, jnp.int32),
            pltpu.VMEM((2 * block, LANES), jnp.int32),
            pltpu.VMEM((2 * block, LANES), jnp.float32),
            pltpu.VMEM((2 * block, LANES), jnp.float32),
            pltpu.VMEM((2 * block, LANES), jnp.float32),
            pltpu.VMEM((groups, 4, 2 * block), jnp.float32),
            pltpu.VMEM((2, 4, 2 * block), jnp.float32),
            pltpu.VMEM((nv, 4, 2 * block), jnp.float32),
            pltpu.VMEM((2 * nv, 4, 2 * block), jnp.float32),
            dma((2, AHEAD + 1)), dma, dma, dma, dma((nv,)), dma, dma,
            dma((2,)), dma((2, ring)), dma((2,)), dma((2, ring)),
            dma, dma((2,)), dma, dma, dma, dma,
        ],
        compiler_params=pltpu.CompilerParams(
            collective_id=0, has_side_effects=True, vmem_limit_bytes=60 * 1024 * 1024
        ),
    )(hidden, head_weight, targets)
    norm, chosen = result[:depths], result[depths:]
    return norm - chosen, norm * norm


def solution(mesh):
    return jax.shard_map(
        functools.partial(body, mesh.shape["hid"], mesh.shape["vocab"]),
        mesh=mesh,
        in_specs=(P(None, "vocab", "hid"), P("hid", "vocab"), P(None, "hid")),
        out_specs=(P(None, "hid"), P(None, "hid")),
        check_vma=False,
    )
```
